8 devices in a mesh: rep: 2 (over z, y), shard: 4 (over x, core).
Axes of the slice: x: 2, y: 2, z: 1, core: 2. Of those that a mesh axis runs over, the one named last changes fastest.
Arguments:
- ratings: float32 [6912, 128], P(('rep', 'shard')), parts along dimension 0
- obs_mask: int32 [6912, 128], P(('rep', 'shard')), parts along dimension 0
- step_counts: int32 [8, 4], P(('rep', 'shard')), parts along dimension 0
- user_init: float32 [6912, 128], P(('rep', 'shard')), parts along dimension 0
- item_init: float32 [256, 128], P(('rep', 'shard')), parts along dimension 0
Outputs:
- output 1: float32 [6912, 128], P(('rep', 'shard')), parts along dimension 0
- output 2: float32 [256, 128], P(('rep', 'shard')), parts along dimension 0
There are 2 independent parts. The reference program is written for one: setup_inputs(seed, part) draws one part's arguments, and reference() takes and returns one part's arrays. A program takes and returns all parts, laid end to end along the dimension named above; each array names one.
All inputs are finite; a program needn't handle non-finite values.
Results may differ from the reference program's by a relative error of at most 0.00147923.
Values are sent between devices in bfloat16 or wider.
A program may use at most 1 GiB of HBM per device.

```python
import math
import jax
import jax.numpy as jnp
from jax import lax

GROUP_SIZE = 4
FACTOR_RANK = 128
ASPECT = 27
ITEMS_DEV = 32
STEPS_MAX = 6
EPOCHS = 2

USERS_DEV = ASPECT * ITEMS_DEV
NUM_USERS = GROUP_SIZE * USERS_DEV
NUM_ITEMS = GROUP_SIZE * ITEMS_DEV
TRUE_RANK = FACTOR_RANK // 4
STEP_SIZE = 0.4 * math.sqrt(FACTOR_RANK) / (USERS_DEV + FACTOR_RANK)
DECAY_RATE = 0.1 * ITEMS_DEV / math.sqrt(FACTOR_RANK)


def draw_layout(layout_key):
    key_list = jax.random.split(layout_key, 5)
    density_pct = jax.random.randint(key_list[0], (GROUP_SIZE, 1, GROUP_SIZE, 1), 10, 41)
    coin_draws = jax.random.randint(key_list[1], (GROUP_SIZE, USERS_DEV, GROUP_SIZE, ITEMS_DEV), 0, 100)
    obs_mask = (coin_draws < density_pct).astype(jnp.int32).reshape(NUM_USERS, NUM_ITEMS)
    slot_count = GROUP_SIZE * GROUP_SIZE
    step_flat = jax.random.randint(key_list[2], (slot_count,), 1, STEPS_MAX + 1)
    top_pos = jax.random.randint(key_list[3], (), 0, slot_count)
    low_pos = (top_pos + 1 + jax.random.randint(key_list[4], (), 0, slot_count - 1)) % slot_count
    slot_ids = jnp.arange(slot_count)
    step_flat = jnp.where(slot_ids == top_pos, STEPS_MAX, jnp.where(slot_ids == low_pos, 1, step_flat))
    return obs_mask, step_flat.reshape(GROUP_SIZE, GROUP_SIZE).astype(jnp.int32)


def setup_inputs(seed: int = 0, part: int = 0) -> dict:
    base_key = jax.random.fold_in(jax.random.key(seed), part)
    key_list = jax.random.split(base_key, 6)
    user_true = jax.random.normal(key_list[0], (NUM_USERS, TRUE_RANK), jnp.float32)
    item_true = jax.random.normal(key_list[1], (NUM_ITEMS, TRUE_RANK), jnp.float32)
    noise_term = 0.3 * jax.random.normal(key_list[2], (NUM_USERS, NUM_ITEMS), jnp.float32)
    ratings = jnp.dot(user_true, item_true.T) / math.sqrt(TRUE_RANK) + noise_term
    obs_mask, step_counts = draw_layout(key_list[3])
    factor_scale = FACTOR_RANK ** -0.25
    user_init = factor_scale * jax.random.normal(key_list[4], (NUM_USERS, FACTOR_RANK), jnp.float32)
    item_init = factor_scale * jax.random.normal(key_list[5], (NUM_ITEMS, FACTOR_RANK), jnp.float32)
    return {"ratings": ratings, "obs_mask": obs_mask, "step_counts": step_counts, "user_init": user_init, "item_init": item_init}


def reference(ratings, obs_mask, step_counts, user_init, item_init):
    rating_blocks = ratings.reshape(GROUP_SIZE, USERS_DEV, GROUP_SIZE, ITEMS_DEV)
    mask_blocks = obs_mask.reshape(GROUP_SIZE, USERS_DEV, GROUP_SIZE, ITEMS_DEV)
    user_blocks = user_init.reshape(GROUP_SIZE, USERS_DEV, FACTOR_RANK)
    item_blocks = item_init.reshape(GROUP_SIZE, ITEMS_DEV, FACTOR_RANK)
    row_ids = jnp.arange(GROUP_SIZE)

    def block_update(block_args):
        row_id, col_id, user_blk, item_blk = block_args
        rating_blk = rating_blocks[row_id, :, col_id, :]
        seen_blk = mask_blocks[row_id, :, col_id, :] != 0

        def grad_step(step_idx, inner_in):
            user_now, item_now = inner_in
            user_half = user_now.astype(jnp.bfloat16)
            item_half = item_now.astype(jnp.bfloat16)
            approx = jnp.dot(user_half, item_half.T, preferred_element_type=jnp.float32)
            err_half = jnp.where(seen_blk, approx - rating_blk, 0.0).astype(jnp.bfloat16)
            grad_user = jnp.dot(err_half, item_half, preferred_element_type=jnp.float32) + DECAY_RATE * user_now
            grad_item = jnp.dot(err_half.T, user_half, preferred_element_type=jnp.float32) + DECAY_RATE * item_now
            return user_now - STEP_SIZE * grad_user, item_now - STEP_SIZE * grad_item

        return lax.fori_loop(0, step_counts[row_id, col_id], grad_step, (user_blk, item_blk))

    def sub_epoch(sweep_idx, carry_in):
        user_cur, held_items = carry_in
        col_ids = (row_ids + sweep_idx) % GROUP_SIZE
        user_new, item_new = lax.map(block_update, (row_ids, col_ids, user_cur, held_items))
        return user_new, jnp.roll(item_new, -1, axis=0)

    user_fin, item_fin = lax.fori_loop(0, EPOCHS * GROUP_SIZE, sub_epoch, (user_blocks, item_blocks))
    return user_fin.reshape(NUM_USERS, FACTOR_RANK), item_fin.reshape(NUM_ITEMS, FACTOR_RANK)
```

```python
import math
import jax
import jax.numpy as jnp
from jax import lax
from jax.sharding import PartitionSpec as P
from jax.experimental import pallas as pl
from jax.experimental.pallas import tpu as pltpu

EPOCHS = 2
STEPS_MAX = 6
MESH = pl.DeviceIdType.MESH
PIECE = 32


def solution(mesh):
    group_size = mesh.shape["shard"]
    row_spec = P(("rep", "shard"), None)
    sweeps = EPOCHS * group_size
    half = jnp.bfloat16

    def local_run(ratings, obs_mask, step_counts, user_init, item_init):
        users_dev, rank_dim = user_init.shape
        items_dev = item_init.shape[0]
        step_size = 0.4 * math.sqrt(rank_dim) / (users_dev + rank_dim)
        decay_rate = 0.1 * items_dev / math.sqrt(rank_dim)
        shrink = 1.0 - step_size * decay_rate
        blocks = -(-users_dev // 128)
        last_rows = users_dev - 128 * (blocks - 1)

        def place(block):
            return block // 4, (block // 2) % 2, block % 2

        def rows_of(ref, block):
            if block < blocks - 1 or last_rows == 128:
                return ref[pl.ds(128 * block, 128), :]
            tail = ref[pl.ds(128 * block, last_rows), :]
            return jnp.concatenate([tail, jnp.zeros((128 - last_rows, tail.shape[1]), tail.dtype)], axis=0)

        def sweep_kernel(counts, rating_hbm, mask_hbm, user_hbm, item_hbm, ut_out, item_out,
                         rating_in, mask_in, user_in, item_in, rt, mt, ut, uth, item_sent, load_sem, send_sem, recv_sem):
            me = lax.axis_index("shard")
            left = lax.rem(me + group_size - 1, group_size)
            right = lax.rem(me + 1, group_size)
            loads = [
                pltpu.make_async_copy(user_hbm, user_in, load_sem.at[0]),
                pltpu.make_async_copy(rating_hbm, rating_in, load_sem.at[1]),
                pltpu.make_async_copy(mask_hbm, mask_in, load_sem.at[2]),
                pltpu.make_async_copy(item_hbm, item_in.at[0], load_sem.at[3]),
            ]
            for load in loads:
                load.start()
            barrier = pltpu.get_barrier_semaphore()
            for neighbour in (left, right):
                pl.semaphore_signal(barrier, inc=1, device_id={"shard": neighbour}, device_id_type=MESH)

            loads[0].wait()
            ut[...] = jnp.zeros_like(ut)
            uth[...] = jnp.zeros_like(uth)
            rt[...] = jnp.zeros_like(rt)
            mt[...] = jnp.zeros_like(mt)
            for b in range(blocks):
                m, h, s = place(b)
                blk = rows_of(user_in, b).T
                ut[m, pl.ds(128 * h, 128), pl.ds(128 * s, 128)] = blk
                uth[m, pl.ds(128 * h, 128), pl.ds(128 * s, 128)] = blk.astype(half)
            loads[1].wait()
            for b in range(blocks):
                m, h, s = place(b)
                blk = rows_of(rating_in, b).T
                for j in range(group_size):
                    rt[m, j, pl.ds(items_dev * h, items_dev), pl.ds(128 * s, 128)] = blk[items_dev * j:items_dev * (j + 1)]
            loads[2].wait()
            for b in range(blocks):
                m, h, s = place(b)
                blk = rows_of(mask_in, b).T
                for j in range(group_size):
                    mt[m, j, pl.ds(items_dev * h, items_dev), pl.ds(128 * s, 128)] = blk[items_dev * j:items_dev * (j + 1)]
            loads[3].wait()
            pl.semaphore_wait(barrier, 2)

            lane = lax.broadcasted_iota(jnp.int32, (128, 128), 1)
            pair = 2 * items_dev

            def one_step(item_now, col, active):
                threshold = jnp.where(active, 0, 1)
                keep = jnp.where(active, jnp.float32(shrink), jnp.float32(1.0))
                item_half = item_now.astype(half)
                none = jnp.zeros_like(item_half)
                lhs_a = jnp.concatenate([
                    jnp.concatenate([item_half, none], axis=1),
                    jnp.concatenate([none, item_half], axis=1)], axis=0)
                item_t = jnp.concatenate(
                    [item_now, item_now, jnp.zeros((128 - pair, rank_dim), jnp.float32)], axis=0).T
                top = jnp.where(lane < items_dev, item_t, 0.0).astype(half)
                low = jnp.where((lane >= items_dev) & (lane < pair), item_t, 0.0).astype(half)
                lhs_u = jnp.concatenate([top, low], axis=0)[:, :pair]
                errs = []
                for m in range(2):
                    approx = jnp.dot(lhs_a, uth[m], preferred_element_type=jnp.float32)
                    seen = mt[m, col] > threshold
                    errs.append(jnp.where(seen, approx - rt[m, col], 0.0).astype(half))
                grads = [lax.dot_general(errs[m], uth[m], (((1,), (1,)), ((), ())), preferred_element_type=jnp.float32) for m in range(2)]
                grad_item = ((grads[0][:items_dev, :128] + grads[0][items_dev:, 128:])
                             + (grads[1][:items_dev, :128] + grads[1][items_dev:, 128:]))
                item_new = keep * item_now - step_size * grad_item
                for m in range(2):
                    grad = jnp.dot(lhs_u, errs[m], preferred_element_type=jnp.float32)
                    fresh = keep * ut[m] - step_size * grad
                    ut[m] = fresh
                    uth[m] = fresh.astype(half)
                return item_new

            def sub_epoch(t, carry):
                col = lax.rem(me + t, group_size)
                count = counts[0, col]
                item_now = item_in[t]
                for k in range(STEPS_MAX):
                    item_now = one_step(item_now, col, k < count)
                item_sent[t] = item_now
                hop = pltpu.make_async_remote_copy(
                    src_ref=item_sent.at[t], dst_ref=item_in.at[t + 1],
                    send_sem=send_sem.at[t], recv_sem=recv_sem.at[t],
                    device_id={"shard": left}, device_id_type=MESH)
                hop.start()
                hop.wait()
                return carry

            lax.fori_loop(0, sweeps, sub_epoch, 0)
            ut_out[...] = ut[...]
            item_out[...] = item_in[sweeps]

        vmem = pl.BlockSpec(memory_space=pltpu.VMEM)
        ut_fin, item_fin = pl.pallas_call(
            sweep_kernel,
            out_shape=(jax.ShapeDtypeStruct((2, 256, 256), jnp.float32), jax.ShapeDtypeStruct(item_init.shape, jnp.float32)),
            in_specs=[pl.BlockSpec(memory_space=pltpu.SMEM)] + [pl.BlockSpec(memory_space=pl.ANY)] * 4,
            out_specs=(vmem, vmem),
            scratch_shapes=[
                pltpu.VMEM(ratings.shape, jnp.float32),
                pltpu.VMEM(obs_mask.shape, jnp.int32),
                pltpu.VMEM(user_init.shape, jnp.float32),
                pltpu.VMEM((sweeps + 1,) + item_init.shape, jnp.float32),
                pltpu.VMEM((2, group_size, 2 * items_dev, 256), jnp.float32),
                pltpu.VMEM((2, group_size, 2 * items_dev, 256), jnp.int32),
                pltpu.VMEM((2, 256, 256), jnp.float32),
                pltpu.VMEM((2, 256, 256), half),
                pltpu.VMEM((sweeps,) + item_init.shape, jnp.float32),
                pltpu.SemaphoreType.DMA((4,)),
                pltpu.SemaphoreType.DMA((sweeps,)),
                pltpu.SemaphoreType.DMA((sweeps,)),
            ],
            compiler_params=pltpu.CompilerParams(collective_id=0, has_side_effects=True),
            name="sweeps",
        )(step_counts, ratings, obs_mask, user_init, item_init)

        def finish_kernel(ut_ref, item_ref, user_out, item_out):
            for b in range(blocks):
                m, h, s = place(b)
                blk = ut_ref[m, pl.ds(128 * h, 128), pl.ds(128 * s, 128)].T
                rows = min(128, users_dev - 128 * b)
                user_out[pl.ds(128 * b, rows), :] = blk[:rows]
            item_out[...] = item_ref[...]

        return pl.pallas_call(
            finish_kernel,
            out_shape=(jax.ShapeDtypeStruct(user_init.shape, jnp.float32), jax.ShapeDtypeStruct(item_init.shape, jnp.float32)),
            in_specs=[vmem, vmem],
            out_specs=(vmem, vmem),
            name="finish",
        )(ut_fin, item_fin)

    return jax.shard_map(local_run, mesh=mesh, in_specs=(row_spec,) * 5, out_specs=(row_spec, row_spec), check_vma=False)
```

```python
import math
import jax
import jax.numpy as jnp
from jax import lax
from jax.sharding import PartitionSpec as P
from jax.experimental import pallas as pl
from jax.experimental.pallas import tpu as pltpu

EPOCHS = 2
STEPS_MAX = 6
MESH = pl.DeviceIdType.MESH
LANES = 128
GROUP = 256


def solution(mesh):
    group_size = mesh.shape["shard"]
    row_spec = P(("rep", "shard"), None)
    sweeps = EPOCHS * group_size
    half = jnp.bfloat16
    full = jnp.float32

    def local_run(ratings, obs_mask, step_counts, user_init, item_init):
        users_dev, rank_dim = user_init.shape
        items_dev = item_init.shape[0]
        step_size = 0.4 * math.sqrt(rank_dim) / (users_dev + rank_dim)
        decay_rate = 0.1 * items_dev / math.sqrt(rank_dim)
        shrink = 1.0 - step_size * decay_rate
        blocks = -(-users_dev // LANES)
        groups = -(-users_dev // GROUP)
        biggest = float(jnp.finfo(full).max)

        def rows_of(ref, block):
            rows = min(LANES, users_dev - LANES * block)
            part = ref[pl.ds(LANES * block, rows), :]
            if rows == LANES:
                return part
            return jnp.concatenate([part, jnp.zeros((LANES - rows, part.shape[1]), part.dtype)], axis=0)

        def sweep_kernel(counts_hbm, rating_hbm, mask_hbm, user_hbm, item_hbm, user_out, item_out,
                         counts, rating_in, mask_in, user_in, item_in, item_sent, rt, ut, uth, load_sem, send_sem, recv_sem):
            me = lax.axis_index("shard")
            left = lax.rem(me + group_size - 1, group_size)
            right = lax.rem(me + 1, group_size)
            load_user = pltpu.make_async_copy(user_hbm, user_in, load_sem.at[0])
            load_rating = pltpu.make_async_copy(rating_hbm, rating_in, load_sem.at[1])
            load_mask = pltpu.make_async_copy(mask_hbm, mask_in, load_sem.at[2])
            load_counts = pltpu.make_async_copy(counts_hbm, counts, load_sem.at[3])
            load_item = pltpu.make_async_copy(item_hbm, item_in.at[0], recv_sem.at[0])
            for load in (load_user, load_rating, load_mask, load_counts, load_item):
                load.start()
            barrier = pltpu.get_barrier_semaphore()
            for neighbour in (left, right):
                pl.semaphore_signal(barrier, inc=1, device_id={"shard": neighbour}, device_id_type=MESH)

            spare = GROUP * groups - LANES * blocks
            if spare:
                ut[groups - 1, :, pl.ds(GROUP - spare, spare)] = jnp.zeros((rank_dim, spare), full)
                uth[groups - 1, :, pl.ds(GROUP - spare, spare)] = jnp.zeros((rank_dim, spare), half)
                for j in range(group_size):
                    rt[j, groups - 1, :, pl.ds(GROUP - spare, spare)] = jnp.full((items_dev, spare), jnp.nan, full)
            load_user.wait()
            for b in range(blocks):
                g, s = divmod(b * LANES, GROUP)
                blk = rows_of(user_in, b).T
                ut[g, :, pl.ds(s, LANES)] = blk
                uth[g, :, pl.ds(s, LANES)] = blk.astype(half)
            load_rating.wait()
            load_mask.wait()
            for b in range(blocks):
                g, s = divmod(b * LANES, GROUP)
                blk = jnp.where(rows_of(mask_in, b) != 0, rows_of(rating_in, b), jnp.nan).T
                for j in range(group_size):
                    rt[j, g, :, pl.ds(s, LANES)] = blk[items_dev * j:items_dev * (j + 1)]
            load_counts.wait()
            pl.semaphore_wait(barrier, 2)

            def errors(item_now, col, limit):
                item_half = item_now.astype(half)
                errs = []
                for g in range(groups):
                    approx = jnp.dot(item_half, uth[g], preferred_element_type=full)
                    rating = rt[col, g]
                    errs.append(jnp.where(rating <= limit, approx - rating, 0.0).astype(half))
                return errs

            def next_item(item_now, errs, keep):
                grad = None
                for g in range(0, groups, 2):
                    both = jnp.concatenate(errs[g:g + 2], axis=0)
                    users = jnp.concatenate([uth[g], uth[g + 1]], axis=0)
                    prod = lax.dot_general(both, users, (((1,), (1,)), ((), ())), preferred_element_type=full)
                    part = prod[:items_dev, :rank_dim] + prod[items_dev:, rank_dim:]
                    grad = part if grad is None else grad + part
                return keep * item_now - step_size * grad

            def update_users(item_now, errs, keep):
                item_t = item_now.T.astype(half)
                for g in range(groups):
                    grad = jnp.dot(item_t, errs[g], preferred_element_type=full)
                    fresh = keep * ut[g] - step_size * grad
                    ut[g] = fresh
                    uth[g] = fresh.astype(half)

            def hop(t):
                return pltpu.make_async_remote_copy(
                    src_ref=item_sent.at[t], dst_ref=item_in.at[t + 1],
                    send_sem=send_sem.at[t], recv_sem=recv_sem.at[t + 1],
                    device_id={"shard": left}, device_id_type=MESH)

            def arrived(t):
                return pltpu.make_async_copy(item_in.at[t], item_in.at[t], recv_sem.at[t])

            def sub_epoch(t, carry):
                col = lax.rem(me + t, group_size)
                count = counts[0, col]
                arrived(t).wait()
                item_now = item_in[t]
                for k in range(STEPS_MAX):
                    limit = jnp.where(k < count, full(biggest), full(-jnp.inf))
                    keep = jnp.where(k < count, full(shrink), full(1.0))
                    errs = errors(item_now, col, limit)
                    item_new = next_item(item_now, errs, keep)
                    if k == STEPS_MAX - 1:
                        item_sent[t] = item_new
                        hop(t).start()
                    update_users(item_now, errs, keep)
                    item_now = item_new
                return carry

            lax.fori_loop(0, sweeps, sub_epoch, 0)
            for b in range(blocks):
                g, s = divmod(b * LANES, GROUP)
                rows = min(LANES, users_dev - LANES * b)
                user_out[pl.ds(LANES * b, rows), :] = ut[g, :, pl.ds(s, LANES)].T[:rows]
            for t in range(sweeps):
                hop(t).wait_send()
            arrived(sweeps).wait()
            item_out[...] = item_in[sweeps]

        vmem = pl.BlockSpec(memory_space=pltpu.VMEM)
        hbm = pl.BlockSpec(memory_space=pl.ANY)
        user_fin, item_fin = pl.pallas_call(
            sweep_kernel,
            out_shape=(pltpu.VMEM(user_init.shape, full), pltpu.VMEM(item_init.shape, full)),
            in_specs=[hbm] * 5,
            out_specs=(vmem, vmem),
            scratch_shapes=[
                pltpu.SMEM(step_counts.shape, jnp.int32),
                pltpu.VMEM(ratings.shape, full),
                pltpu.VMEM(obs_mask.shape, jnp.int32),
                pltpu.VMEM(user_init.shape, full),
                pltpu.VMEM((sweeps + 1,) + item_init.shape, full),
                pltpu.VMEM((sweeps,) + item_init.shape, full),
                pltpu.VMEM((group_size, groups, items_dev, GROUP), full),
                pltpu.VMEM((groups, rank_dim, GROUP), full),
                pltpu.VMEM((groups, rank_dim, GROUP), half),
                pltpu.SemaphoreType.DMA((4,)),
                pltpu.SemaphoreType.DMA((sweeps,)),
                pltpu.SemaphoreType.DMA((sweeps + 1,)),
            ],
            compiler_params=pltpu.CompilerParams(collective_id=0, has_side_effects=True),
            name="sweeps",
        )(step_counts, ratings, obs_mask, user_init, item_init)

        user_fin, item_fin = (pltpu.with_memory_space_constraint(x, pltpu.VMEM) for x in (user_fin, item_fin))

        def finish_kernel(user_ref, item_ref, user_out, item_out, sem):
            copies = [pltpu.make_async_copy(user_ref, user_out, sem.at[0]), pltpu.make_async_copy(item_ref, item_out, sem.at[1])]
            for copy in copies:
                copy.start()
            for copy in copies:
                copy.wait()

        return pl.pallas_call(
            finish_kernel,
            out_shape=(jax.ShapeDtypeStruct(user_init.shape, full), jax.ShapeDtypeStruct(item_init.shape, full)),
            in_specs=[vmem, vmem],
            out_specs=(hbm, hbm),
            scratch_shapes=[pltpu.SemaphoreType.DMA((2,))],
            name="finish",
        )(user_fin, item_fin)

    return jax.shard_map(local_run, mesh=mesh, in_specs=(row_spec,) * 5, out_specs=(row_spec, row_spec), check_vma=False)
```

```python
import math
import jax
import jax.numpy as jnp
from jax import lax
from jax.sharding import PartitionSpec as P
from jax.experimental import pallas as pl
from jax.experimental.pallas import tpu as pltpu

EPOCHS = 2
STEPS_MAX = 6
MESH = pl.DeviceIdType.MESH
LANES = 128
GROUP = 256


def solution(mesh):
    group_size = mesh.shape["shard"]
    row_spec = P(("rep", "shard"), None)
    sweeps = EPOCHS * group_size
    half = jnp.bfloat16
    full = jnp.float32

    def local_run(ratings, obs_mask, step_counts, user_init, item_init):
        users_dev, rank_dim = user_init.shape
        items_dev = item_init.shape[0]
        step_size = 0.4 * math.sqrt(rank_dim) / (users_dev + rank_dim)
        decay_rate = 0.1 * items_dev / math.sqrt(rank_dim)
        shrink = 1.0 - step_size * decay_rate
        blocks = -(-users_dev // LANES)
        groups = -(-users_dev // GROUP)
        biggest = float(jnp.finfo(full).max)

        def rows_of(ref, block):
            rows = min(LANES, users_dev - LANES * block)
            part = ref[pl.ds(LANES * block, rows), :]
            if rows == LANES:
                return part
            return jnp.concatenate([part, jnp.zeros((LANES - rows, part.shape[1]), part.dtype)], axis=0)

        def sweep_kernel(counts_hbm, rating_hbm, mask_hbm, user_hbm, item_hbm, user_out, item_out,
                         counts, rating_in, mask_in, user_in, item_in, item_sent, rt, ut, uth, load_sem, send_sem, recv_sem):
            me = lax.axis_index("shard")
            left = lax.rem(me + group_size - 1, group_size)
            right = lax.rem(me + 1, group_size)
            load_user = pltpu.make_async_copy(user_hbm, user_in, load_sem.at[0])
            load_rating = pltpu.make_async_copy(rating_hbm, rating_in, load_sem.at[1])
            load_mask = pltpu.make_async_copy(mask_hbm, mask_in, load_sem.at[2])
            load_counts = pltpu.make_async_copy(counts_hbm, counts, load_sem.at[3])
            load_item = pltpu.make_async_copy(item_hbm, item_in.at[0], recv_sem.at[0])
            for load in (load_user, load_rating, load_mask, load_counts, load_item):
                load.start()
            barrier = pltpu.get_barrier_semaphore()
            for neighbour in (left, right):
                pl.semaphore_signal(barrier, inc=1, device_id={"shard": neighbour}, device_id_type=MESH)

            spare = GROUP * groups - LANES * blocks
            if spare:
                ut[groups - 1, :, pl.ds(GROUP - spare, spare)] = jnp.zeros((rank_dim, spare), full)
                uth[groups - 1, :, pl.ds(GROUP - spare, spare)] = jnp.zeros((rank_dim, spare), half)
                for j in range(group_size):
                    rt[j, groups - 1, :, pl.ds(GROUP - spare, spare)] = jnp.full((items_dev, spare), jnp.nan, full)
            load_user.wait()
            for b in range(blocks):
                g, s = divmod(b * LANES, GROUP)
                blk = rows_of(user_in, b).T
                ut[g, :, pl.ds(s, LANES)] = blk
                uth[g, :, pl.ds(s, LANES)] = blk.astype(half)
            load_rating.wait()
            load_mask.wait()
            for b in range(blocks):
                g, s = divmod(b * LANES, GROUP)
                blk = jnp.where(rows_of(mask_in, b) != 0, rows_of(rating_in, b), jnp.nan).T
                for j in range(group_size):
                    rt[j, g, :, pl.ds(s, LANES)] = blk[items_dev * j:items_dev * (j + 1)]
            load_counts.wait()
            load_item.wait()

            def error(g, item_half, col, limit):
                approx = jnp.dot(item_half, uth[g], preferred_element_type=full)
                rating = rt[col, g]
                return jnp.where(rating <= limit, approx - rating, 0.0).astype(half)

            def grad_pair(a, b, errs):
                both = jnp.concatenate([errs[a], errs[b]], axis=0)
                users = jnp.concatenate([uth[a].T, uth[b].T], axis=1)
                prod = jnp.dot(both, users, preferred_element_type=full)
                return prod[:items_dev, :rank_dim] + prod[items_dev:, rank_dim:]

            def user_grad(g, item_t, errs):
                return jnp.dot(item_t, errs[g], preferred_element_type=full)

            def update(g, grad, keep):
                fresh = keep * ut[g] - step_size * grad
                ut[g] = fresh
                uth[g] = fresh.astype(half)

            def hop(t):
                return pltpu.make_async_remote_copy(
                    src_ref=item_sent.at[t], dst_ref=item_in.at[t + 1],
                    send_sem=send_sem.at[t], recv_sem=recv_sem.at[t + 1],
                    device_id={"shard": left}, device_id_type=MESH)

            def arrived(t):
                return pltpu.make_async_copy(item_in.at[t], item_in.at[t], recv_sem.at[t])

            def sub_epoch(t, first):
                col = lax.rem(me + t, group_size)
                count = counts[0, col]
                if first:
                    item_now = item_in[t]
                    item_half = item_now.astype(half)
                else:
                    arrived(t).wait()
                    item_now = item_in[t]
                    item_half = item_now.astype(half)
                for k in range(STEPS_MAX):
                    limit = jnp.where(k < count, full(biggest), full(-jnp.inf))
                    keep = jnp.where(k < count, full(shrink), full(1.0))
                    item_t = item_half.T
                    errs, user_grads, parts = {}, {}, []
                    errs[0] = error(0, item_half, col, limit)
                    errs[1] = error(1, item_half, col, limit)
                    errs[2] = error(2, item_half, col, limit)
                    errs[3] = error(3, item_half, col, limit)
                    user_grads[0] = user_grad(0, item_t, errs)
                    parts.append(grad_pair(0, 1, errs))
                    parts.append(grad_pair(2, 3, errs))
                    item_now = keep * item_now - step_size * sum(parts[1:], parts[0])
                    half_new = item_now.astype(half)
                    if k == STEPS_MAX - 1:
                        if first:
                            pl.semaphore_wait(barrier, 2)
                        item_sent[t] = item_now
                        hop(t).start()
                    user_grads[1] = user_grad(1, item_t, errs)
                    user_grads[2] = user_grad(2, item_t, errs)
                    user_grads[3] = user_grad(3, item_t, errs)
                    update(0, user_grads[0], keep)
                    update(1, user_grads[1], keep)
                    update(2, user_grads[2], keep)
                    update(3, user_grads[3], keep)
                    item_half = half_new

            def middle(t, carry):
                sub_epoch(t, False)
                return carry

            sub_epoch(0, True)
            lax.fori_loop(1, sweeps, middle, 0)
            for b in range(blocks):
                g, s = divmod(b * LANES, GROUP)
                rows = min(LANES, users_dev - LANES * b)
                user_out[pl.ds(LANES * b, rows), :] = ut[g, :, pl.ds(s, LANES)].T[:rows]
            for t in range(sweeps):
                hop(t).wait_send()
            arrived(sweeps).wait()
            item_out[...] = item_in[sweeps]

        vmem = pl.BlockSpec(memory_space=pltpu.VMEM)
        hbm = pl.BlockSpec(memory_space=pl.ANY)
        user_fin, item_fin = pl.pallas_call(
            sweep_kernel,
            out_shape=(pltpu.VMEM(user_init.shape, full), pltpu.VMEM(item_init.shape, full)),
            in_specs=[hbm] * 5,
            out_specs=(vmem, vmem),
            scratch_shapes=[
                pltpu.SMEM(step_counts.shape, jnp.int32),
                pltpu.VMEM(ratings.shape, full),
                pltpu.VMEM(obs_mask.shape, jnp.int32),
                pltpu.VMEM(user_init.shape, full),
                pltpu.VMEM((sweeps + 1,) + item_init.shape, full),
                pltpu.VMEM((sweeps,) + item_init.shape, full),
                pltpu.VMEM((group_size, groups, items_dev, GROUP), full),
                pltpu.VMEM((groups, rank_dim, GROUP), full),
                pltpu.VMEM((groups, rank_dim, GROUP), half),
                pltpu.SemaphoreType.DMA((4,)),
                pltpu.SemaphoreType.DMA((sweeps,)),
                pltpu.SemaphoreType.DMA((sweeps + 1,)),
            ],
            compiler_params=pltpu.CompilerParams(collective_id=0, has_side_effects=True),
            name="sweeps",
        )(step_counts, ratings, obs_mask, user_init, item_init)

        user_fin, item_fin = (pltpu.with_memory_space_constraint(x, pltpu.VMEM) for x in (user_fin, item_fin))

        def finish_kernel(user_ref, item_ref, user_out, item_out, sem):
            copies = [pltpu.make_async_copy(user_ref, user_out, sem.at[0]), pltpu.make_async_copy(item_ref, item_out, sem.at[1])]
            for copy in copies:
                copy.start()
            for copy in copies:
                copy.wait()

        return pl.pallas_call(
            finish_kernel,
            out_shape=(jax.ShapeDtypeStruct(user_init.shape, full), jax.ShapeDtypeStruct(item_init.shape, full)),
            in_specs=[vmem, vmem],
            out_specs=(hbm, hbm),
            scratch_shapes=[pltpu.SemaphoreType.DMA((2,))],
            name="finish",
        )(user_fin, item_fin)

    return jax.shard_map(local_run, mesh=mesh, in_specs=(row_spec,) * 5, out_specs=(row_spec, row_spec), check_vma=False)
```

```python
import math
import jax
import jax.numpy as jnp
from jax import lax
from jax.sharding import PartitionSpec as P
from jax.experimental import pallas as pl
from jax.experimental.pallas import tpu as pltpu

EPOCHS = 2
STEPS_MAX = 6
MESH = pl.DeviceIdType.MESH
LANES = 128
GROUP = 256


def solution(mesh):
    group_size = mesh.shape["shard"]
    row_spec = P(("rep", "shard"), None)
    sweeps = EPOCHS * group_size
    half = jnp.bfloat16
    full = jnp.float32

    def local_run(ratings, obs_mask, step_counts, user_init, item_init):
        users_dev, rank_dim = user_init.shape
        items_dev = item_init.shape[0]
        step_size = 0.4 * math.sqrt(rank_dim) / (users_dev + rank_dim)
        decay_rate = 0.1 * items_dev / math.sqrt(rank_dim)
        shrink = 1.0 - step_size * decay_rate
        blocks = -(-users_dev // LANES)
        groups = -(-users_dev // GROUP)
        biggest = float(jnp.finfo(full).max)

        def rows_of(ref, block):
            rows = min(LANES, users_dev - LANES * block)
            part = ref[pl.ds(LANES * block, rows), :]
            if rows == LANES:
                return part
            return jnp.concatenate([part, jnp.zeros((LANES - rows, part.shape[1]), part.dtype)], axis=0)

        def sweep_kernel(counts_hbm, rating_hbm, mask_hbm, user_hbm, item_hbm, user_out, item_out,
                         counts, rating_in, mask_in, user_in, item_in, item_sent, rt, ut, uth, load_sem, send_sem, recv_sem):
            me = lax.axis_index("shard")
            left = lax.rem(me + group_size - 1, group_size)
            right = lax.rem(me + 1, group_size)
            load_user = pltpu.make_async_copy(user_hbm, user_in, load_sem.at[0])
            load_rating = pltpu.make_async_copy(rating_hbm, rating_in, load_sem.at[1])
            load_mask = pltpu.make_async_copy(mask_hbm, mask_in, load_sem.at[2])
            load_counts = pltpu.make_async_copy(counts_hbm, counts, load_sem.at[3])
            load_item = pltpu.make_async_copy(item_hbm, item_in.at[0], recv_sem.at[0])
            for load in (load_user, load_rating, load_mask, load_counts, load_item):
                load.start()
            barrier = pltpu.get_barrier_semaphore()
            for neighbour in (left, right):
                pl.semaphore_signal(barrier, inc=1, device_id={"shard": neighbour}, device_id_type=MESH)

            spare = GROUP * groups - LANES * blocks
            if spare:
                uth[groups - 1, :, pl.ds(GROUP - spare, spare)] = jnp.zeros((rank_dim, spare), half)
            load_user.wait()
            for b in range(blocks):
                g, s = divmod(b * LANES, GROUP)
                blk = rows_of(user_in, b).T
                ut[g, :, pl.ds(s, LANES)] = blk
                uth[g, :, pl.ds(s, LANES)] = blk.astype(half)
            load_rating.wait()
            load_mask.wait()
            for b in range(blocks):
                g, s = divmod(b * LANES, GROUP)
                blk = jnp.where(rows_of(mask_in, b) != 0, rows_of(rating_in, b), jnp.nan).T
                for j in range(group_size):
                    rt[j, g, :, pl.ds(s, LANES)] = blk[items_dev * j:items_dev * (j + 1)]
            load_counts.wait()
            load_item.wait()

            def live_of(g):
                return min(GROUP, LANES * blocks - GROUP * g)

            def error(g, item_half, col, limit):
                approx = jnp.dot(item_half, uth[g, :, pl.ds(0, live_of(g))], preferred_element_type=full)
                live = live_of(g)
                rating = rt[col, g, :, pl.ds(0, live)]
                err = jnp.where(rating <= limit, approx - rating, 0.0).astype(half)
                return err

            def grad_deep(gs, errs):
                wide = jnp.concatenate([errs[g] for g in gs], axis=1)
                users = jnp.concatenate([uth[g, :, pl.ds(0, live_of(g))].T for g in gs], axis=0)
                return jnp.dot(wide, users, preferred_element_type=full)

            def user_grad(g, item_t, errs):
                return jnp.dot(item_t, errs[g], preferred_element_type=full)

            def update(g, grad, keep):
                cols = pl.ds(0, live_of(g))
                fresh = keep * ut[g, :, cols] - step_size * grad
                ut[g, :, cols] = fresh
                uth[g, :, cols] = fresh.astype(half)

            def hop(t):
                return pltpu.make_async_remote_copy(
                    src_ref=item_sent.at[t], dst_ref=item_in.at[t + 1],
                    send_sem=send_sem.at[t], recv_sem=recv_sem.at[t + 1],
                    device_id={"shard": left}, device_id_type=MESH)

            def arrived(t):
                return pltpu.make_async_copy(item_in.at[t], item_in.at[t], recv_sem.at[t])

            def sub_epoch(t, first):
                col = lax.rem(me + t, group_size)
                count = counts[0, col]
                if first:
                    item_now = item_in[t]
                    item_half = item_now.astype(half)
                else:
                    arrived(t).wait()
                    item_now = item_in[t]
                    item_half = item_now.astype(half)
                for k in range(STEPS_MAX):
                    limit = jnp.where(k < count, full(biggest), full(-jnp.inf))
                    keep = jnp.where(k < count, full(shrink), full(1.0))
                    item_t = item_half.T
                    errs, user_grads, parts = {}, {}, []
                    errs[2] = error(2, item_half, col, limit)
                    errs[0] = error(0, item_half, col, limit)
                    errs[3] = error(3, item_half, col, limit)
                    errs[1] = error(1, item_half, col, limit)
                    parts.append(grad_deep((0, 1), errs))
                    user_grads[2] = user_grad(2, item_t, errs)
                    parts.append(grad_deep((2, 3), errs))
                    item_now = keep * item_now - step_size * sum(parts[1:], parts[0])
                    half_new = item_now.astype(half)
                    if k == STEPS_MAX - 1:
                        if first:
                            pl.semaphore_wait(barrier, 2)
                        item_sent[t] = item_now
                        hop(t).start()
                    user_grads[0] = user_grad(0, item_t, errs)
                    user_grads[3] = user_grad(3, item_t, errs)
                    user_grads[1] = user_grad(1, item_t, errs)
                    update(2, user_grads[2], keep)
                    update(0, user_grads[0], keep)
                    update(3, user_grads[3], keep)
                    update(1, user_grads[1], keep)
                    item_half = half_new

            def middle(t, carry):
                sub_epoch(t, False)
                return carry

            sub_epoch(0, True)
            lax.fori_loop(1, sweeps, middle, 0)
            for b in range(blocks):
                g, s = divmod(b * LANES, GROUP)
                rows = min(LANES, users_dev - LANES * b)
                user_out[pl.ds(LANES * b, rows), :] = ut[g, :, pl.ds(s, LANES)].T[:rows]
            for t in range(sweeps):
                hop(t).wait_send()
            arrived(sweeps).wait()
            item_out[...] = item_in[sweeps]

        vmem = pl.BlockSpec(memory_space=pltpu.VMEM)
        hbm = pl.BlockSpec(memory_space=pl.ANY)
        user_fin, item_fin = pl.pallas_call(
            sweep_kernel,
            out_shape=(pltpu.VMEM(user_init.shape, full), pltpu.VMEM(item_init.shape, full)),
            in_specs=[hbm] * 5,
            out_specs=(vmem, vmem),
            scratch_shapes=[
                pltpu.SMEM(step_counts.shape, jnp.int32),
                pltpu.VMEM(ratings.shape, full),
                pltpu.VMEM(obs_mask.shape, jnp.int32),
                pltpu.VMEM(user_init.shape, full),
                pltpu.VMEM((sweeps + 1,) + item_init.shape, full),
                pltpu.VMEM((sweeps,) + item_init.shape, full),
                pltpu.VMEM((group_size, groups, items_dev, GROUP), full),
                pltpu.VMEM((groups, rank_dim, GROUP), full),
                pltpu.VMEM((groups, rank_dim, GROUP), half),
                pltpu.SemaphoreType.DMA((4,)),
                pltpu.SemaphoreType.DMA((sweeps,)),
                pltpu.SemaphoreType.DMA((sweeps + 1,)),
            ],
            compiler_params=pltpu.CompilerParams(collective_id=0, has_side_effects=True),
            name="sweeps",
        )(step_counts, ratings, obs_mask, user_init, item_init)

        user_fin, item_fin = (pltpu.with_memory_space_constraint(x, pltpu.VMEM) for x in (user_fin, item_fin))

        def finish_kernel(user_ref, item_ref, user_out, item_out, sem):
            copies = [pltpu.make_async_copy(user_ref, user_out, sem.at[0]), pltpu.make_async_copy(item_ref, item_out, sem.at[1])]
            for copy in copies:
                copy.start()
            for copy in copies:
                copy.wait()

        return pl.pallas_call(
            finish_kernel,
            out_shape=(jax.ShapeDtypeStruct(user_init.shape, full), jax.ShapeDtypeStruct(item_init.shape, full)),
            in_specs=[vmem, vmem],
            out_specs=(hbm, hbm),
            scratch_shapes=[pltpu.SemaphoreType.DMA((2,))],
            name="finish",
        )(user_fin, item_fin)

    return jax.shard_map(local_run, mesh=mesh, in_specs=(row_spec,) * 5, out_specs=(row_spec, row_spec), check_vma=False)
```

```python
import math
import jax
import jax.numpy as jnp
from jax import lax
from jax.sharding import PartitionSpec as P
from jax.experimental import pallas as pl
from jax.experimental.pallas import tpu as pltpu

EPOCHS = 2
STEPS_MAX = 6
MESH = pl.DeviceIdType.MESH
LANES = 128


def solution(mesh):
    group_size = mesh.shape["shard"]
    row_spec = P(("rep", "shard"), None)
    sweeps = EPOCHS * group_size
    half = jnp.bfloat16
    full = jnp.float32

    def local_run(ratings, obs_mask, step_counts, user_init, item_init):
        users_dev, rank_dim = user_init.shape
        items_dev = item_init.shape[0]
        step_size = 0.4 * math.sqrt(rank_dim) / (users_dev + rank_dim)
        decay_rate = 0.1 * items_dev / math.sqrt(rank_dim)
        shrink = 1.0 - step_size * decay_rate
        blocks = -(-users_dev // LANES)
        spans = ((0, 128), (128, 256), (384, 256), (640, 256))
        groups = len(spans)
        wide_users = LANES * blocks
        biggest = float(jnp.finfo(full).max)

        def rows_of(ref, block):
            rows = min(LANES, users_dev - LANES * block)
            part = ref[pl.ds(LANES * block, rows), :]
            if rows == LANES:
                return part
            return jnp.concatenate([part, jnp.zeros((LANES - rows, part.shape[1]), part.dtype)], axis=0)

        def sweep_kernel(counts_hbm, rating_hbm, mask_hbm, user_hbm, item_hbm, user_out, item_out,
                         counts, rating_in, mask_in, user_in, item_in, item_sent, rt, ut, uth, load_sem, send_sem, recv_sem):
            me = lax.axis_index("shard")
            left = lax.rem(me + group_size - 1, group_size)
            right = lax.rem(me + 1, group_size)
            load_user = pltpu.make_async_copy(user_hbm, user_in, load_sem.at[0])
            load_rating = pltpu.make_async_copy(rating_hbm, rating_in, load_sem.at[1])
            load_mask = pltpu.make_async_copy(mask_hbm, mask_in, load_sem.at[2])
            load_counts = pltpu.make_async_copy(counts_hbm, counts, load_sem.at[3])
            load_item = pltpu.make_async_copy(item_hbm, item_in.at[0], recv_sem.at[0])
            for load in (load_user, load_rating, load_mask, load_counts, load_item):
                load.start()
            barrier = pltpu.get_barrier_semaphore()
            for neighbour in (left, right):
                pl.semaphore_signal(barrier, inc=1, device_id={"shard": neighbour}, device_id_type=MESH)

            load_user.wait()
            for b in range(blocks):
                blk = rows_of(user_in, b).T
                ut[:, pl.ds(b * LANES, LANES)] = blk
                uth[:, pl.ds(b * LANES, LANES)] = blk.astype(half)
            load_rating.wait()
            load_mask.wait()
            for b in range(blocks):
                blk = jnp.where(rows_of(mask_in, b) != 0, rows_of(rating_in, b), jnp.nan).T
                for j in range(group_size):
                    rt[j, :, pl.ds(b * LANES, LANES)] = blk[items_dev * j:items_dev * (j + 1)]
            load_counts.wait()
            load_item.wait()

            def cols_of(g):
                return pl.ds(*spans[g])

            def error(g, item_half, col, limit):
                approx = jnp.dot(item_half, uth[:, cols_of(g)], preferred_element_type=full)
                rating = rt[col, :, cols_of(g)]
                return jnp.where(rating <= limit, approx - rating, 0.0).astype(half)

            def grad_deep(gs, errs):
                wide = jnp.concatenate([errs[g] for g in gs], axis=1)
                users = jnp.concatenate([uth[:, cols_of(g)].T for g in gs], axis=0)
                return jnp.dot(wide, users, preferred_element_type=full)

            def user_grad(g, item_t, errs):
                return jnp.dot(item_t, errs[g], preferred_element_type=full)

            def update(g, grad, keep):
                cols = cols_of(g)
                fresh = keep * ut[:, cols] - step_size * grad
                ut[:, cols] = fresh
                uth[:, cols] = fresh.astype(half)

            def hop(t):
                return pltpu.make_async_remote_copy(
                    src_ref=item_sent.at[t], dst_ref=item_in.at[t + 1],
                    send_sem=send_sem.at[t], recv_sem=recv_sem.at[t + 1],
                    device_id={"shard": left}, device_id_type=MESH)

            def arrived(t):
                return pltpu.make_async_copy(item_in.at[t], item_in.at[t], recv_sem.at[t])

            def sub_epoch(t, first):
                col = lax.rem(me + t, group_size)
                count = counts[0, col]
                if first:
                    item_now = item_in[t]
                    item_half = item_now.astype(half)
                else:
                    arrived(t).wait()
                    item_now = item_in[t]
                    item_half = item_now.astype(half)
                for k in range(STEPS_MAX):
                    limit = jnp.where(k < count, full(biggest), full(-jnp.inf))
                    keep = jnp.where(k < count, full(shrink), full(1.0))
                    item_t = item_half.T
                    errs, user_grads, parts = {}, {}, []
                    errs[2] = error(2, item_half, col, limit)
                    errs[0] = error(0, item_half, col, limit)
                    errs[3] = error(3, item_half, col, limit)
                    errs[1] = error(1, item_half, col, limit)
                    parts.append(grad_deep((0, 1), errs))
                    user_grads[2] = user_grad(2, item_t, errs)
                    parts.append(grad_deep((2, 3), errs))
                    item_now = keep * item_now - step_size * sum(parts[1:], parts[0])
                    half_new = item_now.astype(half)
                    if k == STEPS_MAX - 1:
                        if first:
                            pl.semaphore_wait(barrier, 2)
                        item_sent[t] = item_now
                        hop(t).start()
                    user_grads[0] = user_grad(0, item_t, errs)
                    user_grads[3] = user_grad(3, item_t, errs)
                    user_grads[1] = user_grad(1, item_t, errs)
                    update(2, user_grads[2], keep)
                    update(0, user_grads[0], keep)
                    update(3, user_grads[3], keep)
                    update(1, user_grads[1], keep)
                    item_half = half_new

            def middle(t, carry):
                sub_epoch(t, False)
                return carry

            sub_epoch(0, True)
            lax.fori_loop(1, sweeps, middle, 0)
            for b in range(blocks):
                rows = min(LANES, users_dev - LANES * b)
                user_out[pl.ds(LANES * b, rows), :] = ut[:, pl.ds(b * LANES, LANES)].T[:rows]
            for t in range(sweeps):
                hop(t).wait_send()
            arrived(sweeps).wait()
            item_out[...] = item_in[sweeps]

        vmem = pl.BlockSpec(memory_space=pltpu.VMEM)
        hbm = pl.BlockSpec(memory_space=pl.ANY)
        user_fin, item_fin = pl.pallas_call(
            sweep_kernel,
            out_shape=(pltpu.VMEM(user_init.shape, full), pltpu.VMEM(item_init.shape, full)),
            in_specs=[hbm] * 5,
            out_specs=(vmem, vmem),
            scratch_shapes=[
                pltpu.SMEM(step_counts.shape, jnp.int32),
                pltpu.VMEM(ratings.shape, full),
                pltpu.VMEM(obs_mask.shape, jnp.int32),
                pltpu.VMEM(user_init.shape, full),
                pltpu.VMEM((sweeps + 1,) + item_init.shape, full),
                pltpu.VMEM((sweeps,) + item_init.shape, full),
                pltpu.VMEM((group_size, items_dev, wide_users), full),
                pltpu.VMEM((rank_dim, wide_users), full),
                pltpu.VMEM((rank_dim, wide_users), half),
                pltpu.SemaphoreType.DMA((4,)),
                pltpu.SemaphoreType.DMA((sweeps,)),
                pltpu.SemaphoreType.DMA((sweeps + 1,)),
            ],
            compiler_params=pltpu.CompilerParams(collective_id=0, has_side_effects=True),
            name="sweeps",
        )(step_counts, ratings, obs_mask, user_init, item_init)

        user_fin, item_fin = (pltpu.with_memory_space_constraint(x, pltpu.VMEM) for x in (user_fin, item_fin))

        def finish_kernel(user_ref, item_ref, user_out, item_out, sem):
            copies = [pltpu.make_async_copy(user_ref, user_out, sem.at[0]), pltpu.make_async_copy(item_ref, item_out, sem.at[1])]
            for copy in copies:
                copy.start()
            for copy in copies:
                copy.wait()

        return pl.pallas_call(
            finish_kernel,
            out_shape=(jax.ShapeDtypeStruct(user_init.shape, full), jax.ShapeDtypeStruct(item_init.shape, full)),
            in_specs=[vmem, vmem],
            out_specs=(hbm, hbm),
            scratch_shapes=[pltpu.SemaphoreType.DMA((2,))],
            name="finish",
        )(user_fin, item_fin)

    return jax.shard_map(local_run, mesh=mesh, in_specs=(row_spec,) * 5, out_specs=(row_spec, row_spec), check_vma=False)
```

```python
import math
import jax
import jax.numpy as jnp
from jax import lax
from jax.sharding import PartitionSpec as P
from jax.experimental import pallas as pl
from jax.experimental.pallas import tpu as pltpu

EPOCHS = 2
STEPS_MAX = 6
MESH = pl.DeviceIdType.MESH
LANES = 128


def solution(mesh):
    group_size = mesh.shape["shard"]
    row_spec = P(("rep", "shard"), None)
    sweeps = EPOCHS * group_size
    half = jnp.bfloat16
    full = jnp.float32

    def local_run(ratings, obs_mask, step_counts, user_init, item_init):
        users_dev, rank_dim = user_init.shape
        items_dev = item_init.shape[0]
        step_size = 0.4 * math.sqrt(rank_dim) / (users_dev + rank_dim)
        decay_rate = 0.1 * items_dev / math.sqrt(rank_dim)
        shrink = 1.0 - step_size * decay_rate
        blocks = -(-users_dev // LANES)
        spans = ((0, 128), (128, 256), (384, 256), (640, 256))
        groups = len(spans)
        wide_users = LANES * blocks
        biggest = float(jnp.finfo(full).max)

        def rows_of(ref, block):
            rows = min(LANES, users_dev - LANES * block)
            part = ref[pl.ds(LANES * block, rows), :]
            if rows == LANES:
                return part
            return jnp.concatenate([part, jnp.zeros((LANES - rows, part.shape[1]), part.dtype)], axis=0)

        def sweep_kernel(counts_hbm, rating_hbm, mask_hbm, user_hbm, item_hbm, user_out, item_out,
                         counts, rating_in, mask_in, user_in, item_in, item_sent, rt, ut, uth, load_sem, send_sem, recv_sem):
            me = lax.axis_index("shard")
            left = lax.rem(me + group_size - 1, group_size)
            right = lax.rem(me + 1, group_size)
            load_user = pltpu.make_async_copy(user_hbm, user_in, load_sem.at[0])
            load_rating = pltpu.make_async_copy(rating_hbm, rating_in, load_sem.at[1])
            load_mask = pltpu.make_async_copy(mask_hbm, mask_in, load_sem.at[2])
            load_counts = pltpu.make_async_copy(counts_hbm, counts, load_sem.at[3])
            load_item = pltpu.make_async_copy(item_hbm, item_in.at[0], recv_sem.at[0])
            for load in (load_user, load_rating, load_mask, load_counts, load_item):
                load.start()
            barrier = pltpu.get_barrier_semaphore()
            for neighbour in (left, right):
                pl.semaphore_signal(barrier, inc=1, device_id={"shard": neighbour}, device_id_type=MESH)

            load_user.wait()
            for b in range(blocks):
                blk = rows_of(user_in, b).T
                ut[:, pl.ds(b * LANES, LANES)] = blk
                uth[:, pl.ds(b * LANES, LANES)] = blk.astype(half)
            load_rating.wait()
            load_mask.wait()
            for b in range(blocks):
                blk = jnp.where(rows_of(mask_in, b) != 0, rows_of(rating_in, b), jnp.nan).T
                for j in range(group_size):
                    rt[j, :, pl.ds(b * LANES, LANES)] = blk[items_dev * j:items_dev * (j + 1)]
            load_counts.wait()
            load_item.wait()

            def cols_of(g):
                return pl.ds(*spans[g])

            def error(g, item_half, col, limit):
                approx = jnp.dot(item_half, uth[:, cols_of(g)], preferred_element_type=full)
                rating = rt[col, :, cols_of(g)]
                return jnp.where(rating <= limit, approx - rating, 0.0).astype(half)

            def grad_deep(gs, errs):
                wide = jnp.concatenate([errs[g] for g in gs], axis=1)
                users = jnp.concatenate([uth[:, cols_of(g)].T for g in gs], axis=0)
                return jnp.dot(wide, users, preferred_element_type=full)

            def user_grad(g, item_t, errs):
                return jnp.dot(item_t, errs[g], preferred_element_type=full)

            def update(g, grad, keep):
                cols = cols_of(g)
                old = ut[:, cols]
                fresh = jnp.where(keep, shrink * old - step_size * grad, old)
                ut[:, cols] = fresh
                uth[:, cols] = fresh.astype(half)

            def hop(t):
                return pltpu.make_async_remote_copy(
                    src_ref=item_sent.at[t], dst_ref=item_in.at[t + 1],
                    send_sem=send_sem.at[t], recv_sem=recv_sem.at[t + 1],
                    device_id={"shard": left}, device_id_type=MESH)

            def arrived(t):
                return pltpu.make_async_copy(item_in.at[t], item_in.at[t], recv_sem.at[t])

            def sub_epoch(t, first):
                col = lax.rem(me + t, group_size)
                count = counts[0, col]
                if first:
                    item_now = item_in[t]
                    item_half = item_now.astype(half)
                else:
                    arrived(t).wait()
                    item_now = item_in[t]
                    item_half = item_now.astype(half)
                for k in range(STEPS_MAX):
                    limit = jnp.where(k < count, full(biggest), full(-jnp.inf))
                    keep = k < count
                    item_t = item_half.T
                    errs, user_grads, parts = {}, {}, []
                    errs[2] = error(2, item_half, col, limit)
                    errs[0] = error(0, item_half, col, limit)
                    errs[3] = error(3, item_half, col, limit)
                    errs[1] = error(1, item_half, col, limit)
                    parts.append(grad_deep((0, 1), errs))
                    user_grads[2] = user_grad(2, item_t, errs)
                    parts.append(grad_deep((2, 3), errs))
                    item_now = jnp.where(keep, shrink * item_now - step_size * sum(parts[1:], parts[0]), item_now)
                    half_new = item_now.astype(half)
                    if k == STEPS_MAX - 1:
                        if first:
                            pl.semaphore_wait(barrier, 2)
                        item_sent[t] = item_now
                        hop(t).start()
                    user_grads[0] = user_grad(0, item_t, errs)
                    user_grads[3] = user_grad(3, item_t, errs)
                    user_grads[1] = user_grad(1, item_t, errs)
                    update(2, user_grads[2], keep)
                    update(0, user_grads[0], keep)
                    update(3, user_grads[3], keep)
                    update(1, user_grads[1], keep)
                    item_half = half_new

            def middle(t, carry):
                sub_epoch(t, False)
                return carry

            sub_epoch(0, True)
            lax.fori_loop(1, sweeps, middle, 0)
            for b in range(blocks):
                rows = min(LANES, users_dev - LANES * b)
                user_out[pl.ds(LANES * b, rows), :] = ut[:, pl.ds(b * LANES, LANES)].T[:rows]
            for t in range(sweeps):
                hop(t).wait_send()
            arrived(sweeps).wait()
            item_out[...] = item_in[sweeps]

        vmem = pl.BlockSpec(memory_space=pltpu.VMEM)
        hbm = pl.BlockSpec(memory_space=pl.ANY)
        user_fin, item_fin = pl.pallas_call(
            sweep_kernel,
            out_shape=(pltpu.VMEM(user_init.shape, full), pltpu.VMEM(item_init.shape, full)),
            in_specs=[hbm] * 5,
            out_specs=(vmem, vmem),
            scratch_shapes=[
                pltpu.SMEM(step_counts.shape, jnp.int32),
                pltpu.VMEM(ratings.shape, full),
                pltpu.VMEM(obs_mask.shape, jnp.int32),
                pltpu.VMEM(user_init.shape, full),
                pltpu.VMEM((sweeps + 1,) + item_init.shape, full),
                pltpu.VMEM((sweeps,) + item_init.shape, full),
                pltpu.VMEM((group_size, items_dev, wide_users), full),
                pltpu.VMEM((rank_dim, wide_users), full),
                pltpu.VMEM((rank_dim, wide_users), half),
                pltpu.SemaphoreType.DMA((4,)),
                pltpu.SemaphoreType.DMA((sweeps,)),
                pltpu.SemaphoreType.DMA((sweeps + 1,)),
            ],
            compiler_params=pltpu.CompilerParams(collective_id=0, has_side_effects=True),
            name="sweeps",
        )(step_counts, ratings, obs_mask, user_init, item_init)

        user_fin, item_fin = (pltpu.with_memory_space_constraint(x, pltpu.VMEM) for x in (user_fin, item_fin))

        def finish_kernel(user_ref, item_ref, user_out, item_out, sem):
            copies = [pltpu.make_async_copy(user_ref, user_out, sem.at[0]), pltpu.make_async_copy(item_ref, item_out, sem.at[1])]
            for copy in copies:
                copy.start()
            for copy in copies:
                copy.wait()

        return pl.pallas_call(
            finish_kernel,
            out_shape=(jax.ShapeDtypeStruct(user_init.shape, full), jax.ShapeDtypeStruct(item_init.shape, full)),
            in_specs=[vmem, vmem],
            out_specs=(hbm, hbm),
            scratch_shapes=[pltpu.SemaphoreType.DMA((2,))],
            name="finish",
        )(user_fin, item_fin)

    return jax.shard_map(local_run, mesh=mesh, in_specs=(row_spec,) * 5, out_specs=(row_spec, row_spec), check_vma=False)
```

```python
import math
import jax
import jax.numpy as jnp
from jax import lax
from jax.sharding import PartitionSpec as P
from jax.experimental import pallas as pl
from jax.experimental.pallas import tpu as pltpu

EPOCHS = 2
STEPS_MAX = 6
MESH = pl.DeviceIdType.MESH
LANES = 128


def solution(mesh):
    group_size = mesh.shape["shard"]
    row_spec = P(("rep", "shard"), None)
    sweeps = EPOCHS * group_size
    half = jnp.bfloat16
    full = jnp.float32

    def local_run(ratings, obs_mask, step_counts, user_init, item_init):
        users_dev, rank_dim = user_init.shape
        items_dev = item_init.shape[0]
        step_size = 0.4 * math.sqrt(rank_dim) / (users_dev + rank_dim)
        decay_rate = 0.1 * items_dev / math.sqrt(rank_dim)
        shrink = 1.0 - step_size * decay_rate
        blocks = -(-users_dev // LANES)
        spans = ((0, 128), (128, 256), (384, 256), (640, 256))
        groups = len(spans)
        wide_users = LANES * blocks
        biggest = float(jnp.finfo(full).max)

        def rows_of(ref, block):
            rows = min(LANES, users_dev - LANES * block)
            part = ref[pl.ds(LANES * block, rows), :]
            if rows == LANES:
                return part
            return jnp.concatenate([part, jnp.zeros((LANES - rows, part.shape[1]), part.dtype)], axis=0)

        def sweep_kernel(counts_hbm, rating_hbm, mask_hbm, user_hbm, item_hbm, user_out, item_out,
                         counts, rating_in, mask_in, user_in, item_in, item_sent, rt, ut, uth, load_sem, send_sem, recv_sem):
            me = lax.axis_index("shard")
            left = lax.rem(me + group_size - 1, group_size)
            right = lax.rem(me + 1, group_size)
            load_user = pltpu.make_async_copy(user_hbm, user_in, load_sem.at[0])
            load_rating = pltpu.make_async_copy(rating_hbm, rating_in, load_sem.at[1])
            load_mask = pltpu.make_async_copy(mask_hbm, mask_in, load_sem.at[2])
            load_counts = pltpu.make_async_copy(counts_hbm, counts, load_sem.at[3])
            load_item = pltpu.make_async_copy(item_hbm, item_in.at[0], recv_sem.at[0])
            for load in (load_user, load_rating, load_mask, load_counts, load_item):
                load.start()
            barrier = pltpu.get_barrier_semaphore()
            for neighbour in (left, right):
                pl.semaphore_signal(barrier, inc=1, device_id={"shard": neighbour}, device_id_type=MESH)

            load_user.wait()
            for b in range(blocks):
                blk = rows_of(user_in, b).T
                ut[:, pl.ds(b * LANES, LANES)] = blk
                uth[:, pl.ds(b * LANES, LANES)] = blk.astype(half)
            load_rating.wait()
            load_mask.wait()
            for b in range(blocks):
                blk = jnp.where(rows_of(mask_in, b) != 0, rows_of(rating_in, b), jnp.nan).T
                for j in range(group_size):
                    rt[j, :, pl.ds(b * LANES, LANES)] = blk[items_dev * j:items_dev * (j + 1)]
            load_counts.wait()
            load_item.wait()

            def cols_of(g):
                return pl.ds(*spans[g])

            def error(g, item_half, col, limit):
                approx = jnp.dot(item_half, uth[:, cols_of(g)], preferred_element_type=full)
                rating = rt[col, :, cols_of(g)]
                return jnp.where(rating <= limit, approx - rating, 0.0).astype(half)

            def grad_deep(gs, errs):
                wide = jnp.concatenate([errs[g] for g in gs], axis=1)
                users = jnp.concatenate([uth[:, cols_of(g)].T for g in gs], axis=0)
                return jnp.dot(wide, users, preferred_element_type=full)

            def user_grad(g, item_t, errs):
                return jnp.dot(item_t, errs[g], preferred_element_type=full)

            def update(g, grad, keep):
                cols = cols_of(g)
                fresh = keep * ut[:, cols] - step_size * grad
                ut[:, cols] = fresh
                uth[:, cols] = fresh.astype(half)

            def hop(t):
                return pltpu.make_async_remote_copy(
                    src_ref=item_sent.at[t], dst_ref=item_in.at[t + 1],
                    send_sem=send_sem.at[t], recv_sem=recv_sem.at[t + 1],
                    device_id={"shard": left}, device_id_type=MESH)

            def arrived(t):
                return pltpu.make_async_copy(item_in.at[t], item_in.at[t], recv_sem.at[t])

            def sub_epoch(t, first):
                col = lax.rem(me + t, group_size)
                count = counts[0, col]
                if first:
                    item_now = item_in[t]
                    item_half = item_now.astype(half)
                else:
                    arrived(t).wait()
                    item_now = item_in[t]
                    item_half = item_now.astype(half)
                for k in range(STEPS_MAX):
                    limit = jnp.where(k < count, full(biggest), full(-jnp.inf))
                    keep = jnp.where(k < count, full(shrink), full(1.0))
                    item_t = jnp.where(k < count, item_now, 0.0).astype(half).T
                    errs, user_grads, parts = {}, {}, []
                    errs[2] = error(2, item_half, col, limit)
                    errs[0] = error(0, item_half, col, limit)
                    errs[3] = error(3, item_half, col, limit)
                    errs[1] = error(1, item_half, col, limit)
                    parts.append(grad_deep((0, 1), errs))
                    user_grads[2] = user_grad(2, item_t, errs)
                    parts.append(grad_deep((2, 3), errs))
                    item_now = jnp.where(k < count, keep * item_now - step_size * sum(parts[1:], parts[0]), item_now)
                    half_new = item_now.astype(half)
                    if k == STEPS_MAX - 1:
                        if first:
                            pl.semaphore_wait(barrier, 2)
                        item_sent[t] = item_now
                        hop(t).start()
                    user_grads[0] = user_grad(0, item_t, errs)
                    user_grads[3] = user_grad(3, item_t, errs)
                    user_grads[1] = user_grad(1, item_t, errs)
                    update(2, user_grads[2], keep)
                    update(0, user_grads[0], keep)
                    update(3, user_grads[3], keep)
                    update(1, user_grads[1], keep)
                    item_half = half_new

            def middle(t, carry):
                sub_epoch(t, False)
                return carry

            sub_epoch(0, True)
            lax.fori_loop(1, sweeps, middle, 0)
            for b in range(blocks):
                rows = min(LANES, users_dev - LANES * b)
                user_out[pl.ds(LANES * b, rows), :] = ut[:, pl.ds(b * LANES, LANES)].T[:rows]
            for t in range(sweeps):
                hop(t).wait_send()
            arrived(sweeps).wait()
            item_out[...] = item_in[sweeps]

        vmem = pl.BlockSpec(memory_space=pltpu.VMEM)
        hbm = pl.BlockSpec(memory_space=pl.ANY)
        user_fin, item_fin = pl.pallas_call(
            sweep_kernel,
            out_shape=(pltpu.VMEM(user_init.shape, full), pltpu.VMEM(item_init.shape, full)),
            in_specs=[hbm] * 5,
            out_specs=(vmem, vmem),
            scratch_shapes=[
                pltpu.SMEM(step_counts.shape, jnp.int32),
                pltpu.VMEM(ratings.shape, full),
                pltpu.VMEM(obs_mask.shape, jnp.int32),
                pltpu.VMEM(user_init.shape, full),
                pltpu.VMEM((sweeps + 1,) + item_init.shape, full),
                pltpu.VMEM((sweeps,) + item_init.shape, full),
                pltpu.VMEM((group_size, items_dev, wide_users), full),
                pltpu.VMEM((rank_dim, wide_users), full),
                pltpu.VMEM((rank_dim, wide_users), half),
                pltpu.SemaphoreType.DMA((4,)),
                pltpu.SemaphoreType.DMA((sweeps,)),
                pltpu.SemaphoreType.DMA((sweeps + 1,)),
            ],
            compiler_params=pltpu.CompilerParams(collective_id=0, has_side_effects=True),
            name="sweeps",
        )(step_counts, ratings, obs_mask, user_init, item_init)

        user_fin, item_fin = (pltpu.with_memory_space_constraint(x, pltpu.VMEM) for x in (user_fin, item_fin))

        def finish_kernel(user_ref, item_ref, user_out, item_out, sem):
            copies = [pltpu.make_async_copy(user_ref, user_out, sem.at[0]), pltpu.make_async_copy(item_ref, item_out, sem.at[1])]
            for copy in copies:
                copy.start()
            for copy in copies:
                copy.wait()

        return pl.pallas_call(
            finish_kernel,
            out_shape=(jax.ShapeDtypeStruct(user_init.shape, full), jax.ShapeDtypeStruct(item_init.shape, full)),
            in_specs=[vmem, vmem],
            out_specs=(hbm, hbm),
            scratch_shapes=[pltpu.SemaphoreType.DMA((2,))],
            name="finish",
        )(user_fin, item_fin)

    return jax.shard_map(local_run, mesh=mesh, in_specs=(row_spec,) * 5, out_specs=(row_spec, row_spec), check_vma=False)
```
